32 devices in a mesh: head: 4 (over y, x), seq: 8 (over z, core).
Axes of the slice: x: 2, y: 2, z: 4, core: 2. Of those that a mesh axis runs over, the one named last changes fastest.
Arguments:
- queries: bfloat16 [4, 8192], P(None, ('head', 'seq')), may hold values from -20 to 20
- key_cache: bfloat16 [4, 8, 8192, 128], P(None, 'head', 'seq'), may hold values from -16 to 16
- value_cache: bfloat16 [4, 8, 8192, 128], P(None, 'head', 'seq'), may hold values from -5 to 5
- page_list: int32 [4, 8, 32], P(None, 'head'), may hold values from 0 to 511, as said below
- shard_counts: int32 [4, 8, 8], P(None, 'head'), may hold values from 0 to 8, as said below
- out_weight: bfloat16 [8192, 8192], P(('head', 'seq')), may hold values from -0.125 to 0.125
Outputs:
- output: bfloat16 [4, 8192], P(None, ('head', 'seq'))
- attention: bfloat16 [4, 8192], P(None, ('head', 'seq'))
- page_mass: float32 [4, 64, 512], P(None, 'head', 'seq')
The draws below stay inside these ranges and needn't reach their ends.
Inputs may be any that keep to these rules, and one draw needn't show every extreme that they name: With live = the sum of shard_counts[b, g, :], entries 0 to live - 1 of page_list[b, g] are distinct pages in ascending order, and exactly shard_counts[b, g, s] of them lie in pages s * 64 to (s + 1) * 64 - 1; entries from live on are padding. `shard_counts`: exactly 8 for some index s of every batch row and KV head; the sum over s is at most 32.
All inputs are finite; a program needn't handle non-finite values.
Results may differ from the reference program's by a relative error of at most 0.0052.
Values may be sent and summed in bfloat16 or wider, within the bound.
A program may use at most 64 MiB of HBM per device.

```python
import math
import jax
import jax.numpy as jnp
from jax import lax

D = 8192
HQ = 64
KVH = 8
HD = 128
PAGE = 16
BATCH = 4
CAP = 8
SELECT = 32
PAGES_DEV = 64
CONTEXT = 8192
NPAGES = 512


def selection(key):
    shards = NPAGES // PAGES_DEV
    halves = shards // 2
    streams = jax.random.split(jax.random.fold_in(key, 7001), 6)
    leading = jax.random.randint(streams[0], (BATCH, KVH, halves), 0, CAP + 1)
    forced = jax.random.randint(streams[2], (BATCH, KVH, 1), 0, halves)
    leading = jnp.where(jnp.arange(halves)[None, None, :] == forced, CAP, leading)
    extra = jax.random.randint(streams[1], (BATCH, KVH, halves), 0, CAP + 1)
    trailing = extra % (CAP - leading + 1)
    raw_counts = jnp.concatenate([leading, trailing], axis=2)
    shuffle = jax.random.permutation(streams[3], jnp.broadcast_to(jnp.arange(shards), (BATCH, KVH, shards)), axis=2, independent=True)
    counts = jnp.take_along_axis(raw_counts, shuffle, axis=2).astype(jnp.int32)
    ranks = jax.random.permutation(streams[4], jnp.broadcast_to(jnp.arange(PAGES_DEV), (BATCH, KVH, shards, PAGES_DEV)), axis=3, independent=True)
    flags = (ranks < counts[..., None]).reshape(BATCH, KVH, NPAGES).astype(jnp.int32)
    running = jnp.cumsum(flags, axis=2)
    live_pages = running[:, :, -1]
    slot_ids = jnp.arange(SELECT)
    found = jnp.sum((running[:, :, None, :] <= slot_ids[None, None, :, None]).astype(jnp.int32), axis=3)
    filler = jax.random.randint(streams[5], (BATCH, KVH, SELECT), 0, NPAGES)
    pages = jnp.where(slot_ids[None, None, :] < live_pages[..., None], found, filler).astype(jnp.int32)
    return (counts, pages)


def draw_page_list(key, part):
    return selection(key)[1]


def draw_shard_counts(key, part):
    return selection(key)[0]


def draw_queries(key, part):
    group_size = HQ // KVH
    noise = jnp.clip(jax.random.normal(jax.random.fold_in(key, 11), (BATCH, KVH, group_size, HD), jnp.float32), -4.0, 4.0)
    sample = noise * 2.5
    return jnp.clip(sample, -20.0, 20.0).reshape(BATCH, HQ * HD).astype(jnp.bfloat16)


def draw_key_cache(key, part):
    noise = jnp.clip(jax.random.normal(jax.random.fold_in(key, 21), (BATCH, KVH, CONTEXT, HD), jnp.float32), -4.0, 4.0)
    sample = noise
    return jnp.clip(sample, -16.0, 16.0).astype(jnp.bfloat16)


def raised(array, own_key, source, target, shards_of, factor):
    def block_of(position):
        return (jnp.arange(array.shape[position]) // (array.shape[position] // shards_of)).reshape((-1,) + (1,) * (array.ndim - 1 - position))

    first = jax.random.permutation(own_key, shards_of)[block_of(target)]
    other_side = (block_of(target) + shards_of // 2) % shards_of
    return jnp.where((block_of(source) == first) | (block_of(source) == other_side), factor * array, array)


def block_scale(key, dims, cuts, least, largest):
    loudness = 1.0
    for position, blocks in cuts:
        draws = jax.random.uniform(jax.random.fold_in(jax.random.fold_in(key, 6), position), (blocks,), jnp.float32, least / len(cuts), largest / len(cuts))
        loudness = loudness * jnp.repeat(jnp.exp(draws), dims[position] // blocks).reshape((-1,) + (1,) * (len(dims) - 1 - position))
    return loudness


def normal_values(rng, extent, scale, most, cuts=(), kind=jnp.bfloat16):
    entries = jax.random.normal(rng, extent, jnp.float32) * scale
    if len(cuts) > 0:
        entries = block_scale(rng, extent, cuts, -0.22, 0.18) * entries
    return jnp.clip(entries, min=-most, max=most).astype(kind)


def gaussian_with(key, extent, width, reach, cuts, heavy, kind=jnp.bfloat16):
    drawn = width * jax.random.normal(key, extent, jnp.float32)
    if cuts:
        drawn = drawn * block_scale(key, extent, cuts, -0.22, 0.18)
    return jnp.clip(raised(drawn, jax.random.fold_in(key, 3), *heavy), -reach, reach).astype(kind)


def setup_inputs(seed: int = 0) -> dict:
    key_of = jax.random.split(jax.random.key(seed), 7)
    queries = draw_queries(jax.random.fold_in(key_of[6], 71), 0)
    key_cache = draw_key_cache(jax.random.fold_in(key_of[6], 71), 0)
    value_cache = normal_values(key_of[2], (BATCH, KVH, CONTEXT, HD), 1.0, 5.0, ((1, 4), (2, 8)))
    page_list = draw_page_list(jax.random.fold_in(key_of[6], 71), 0)
    shard_counts = draw_shard_counts(jax.random.fold_in(key_of[6], 71), 0)
    out_weight = gaussian_with(key_of[5], (HQ * HD, D), (HQ * HD) ** -0.5, 0.125, ((0, 32),), (0, 1, 32, 2.75))
    return dict(queries=queries, key_cache=key_cache, value_cache=value_cache, page_list=page_list, shard_counts=shard_counts, out_weight=out_weight)


def pick_pages(table, chosen):
    return table[chosen]

def reference(queries, key_cache, value_cache, page_list, shard_counts, out_weight):
    group_size = HQ // KVH
    score_scale = 1.0 / math.sqrt(HD)
    query_heads = queries.astype(jnp.float32).reshape(BATCH, KVH, group_size, HD)
    live_pages = lax.optimization_barrier(jnp.sum(shard_counts, axis=2))

    def per_head(head_index):
        query_group = lax.dynamic_index_in_dim(query_heads, head_index, 1, keepdims=False)
        head_keys = lax.dynamic_index_in_dim(key_cache, head_index, 1, keepdims=False)
        head_values = lax.dynamic_index_in_dim(value_cache, head_index, 1, keepdims=False)
        head_pages = lax.dynamic_index_in_dim(page_list, head_index, 1, keepdims=False)
        head_live = lax.dynamic_index_in_dim(live_pages, head_index, 1, keepdims=False)
        paged_keys = head_keys.astype(jnp.float32).reshape(BATCH, NPAGES, PAGE, HD)
        lower_keys = lax.optimization_barrier(jnp.min(paged_keys, axis=2))
        upper_keys = lax.optimization_barrier(jnp.max(paged_keys, axis=2))
        page_bound = lax.optimization_barrier(jnp.sum(jnp.maximum(query_group[:, :, None, :] * lower_keys[:, None, :, :], query_group[:, :, None, :] * upper_keys[:, None, :, :]), axis=3)) * score_scale
        page_peak = lax.optimization_barrier(jnp.max(page_bound, axis=2, keepdims=True))
        page_terms = jnp.exp(page_bound - page_peak)
        page_mass = page_terms / lax.optimization_barrier(jnp.sum(page_terms, axis=2, keepdims=True))
        paged_values = head_values.astype(jnp.float32).reshape(BATCH, NPAGES, PAGE, HD)
        chosen_keys = jax.vmap(pick_pages)(paged_keys, head_pages).reshape(BATCH, SELECT * PAGE, HD)
        chosen_values = jax.vmap(pick_pages)(paged_values, head_pages).reshape(BATCH, SELECT * PAGE, HD)
        scores = jnp.einsum('bjd,btd->bjt', query_group, chosen_keys, precision=lax.Precision.HIGHEST) * score_scale
        slot_live = (jnp.arange(SELECT * PAGE, dtype=jnp.int32) // PAGE)[None, :] < head_live[:, None]
        masked = jnp.where(slot_live[:, None, :], scores, -jnp.inf)
        global_top = lax.optimization_barrier(jnp.max(masked, axis=2, keepdims=True))
        weights = jnp.where(slot_live[:, None, :], jnp.exp(masked - global_top), 0.0)
        head_totals = lax.optimization_barrier(jnp.sum(weights, axis=2, keepdims=True))
        rounded = weights.astype(jnp.bfloat16).astype(jnp.float32)
        unnormed = jnp.einsum('bjt,btd->bjd', rounded, chosen_values, precision=lax.Precision.HIGHEST)
        attention = (unnormed / head_totals).astype(jnp.bfloat16)
        return (page_mass, attention)
    masses, attentions = lax.map(per_head, jnp.arange(KVH, dtype=jnp.int32))
    page_mass = jnp.transpose(masses, (1, 0, 2, 3)).reshape(BATCH, HQ, NPAGES)
    attention = jnp.transpose(attentions, (1, 0, 2, 3)).reshape(BATCH, HQ * HD)
    output = jnp.dot(attention, out_weight, preferred_element_type=jnp.float32).astype(jnp.bfloat16)
    return (output, attention, page_mass)
```

```python
import functools
import math

import jax
import jax.numpy as jnp
from jax import lax
from jax.experimental import pallas as pl
from jax.experimental.pallas import tpu as pltpu
from jax.sharding import PartitionSpec as P

HQ = 64
KVH = 8
PAGE = 16
CAP = 8


NEGATIVE = -1e30


def local(queries, key_cache, value_cache, page_list, shard_counts, out_weight):
    batch_rows, kv_local, token_count, head_dim = key_cache.shape
    group_size = HQ // KVH
    pages_local = token_count // PAGE
    shards = lax.axis_size("seq")
    shard_index = lax.axis_index("seq")
    score_scale = 1.0 / math.sqrt(head_dim)
    gathered = lax.all_gather(queries, "seq", axis=1, tiled=True)
    query_heads = gathered.reshape(batch_rows, kv_local, group_size, head_dim)
    page_keys = key_cache.reshape(batch_rows, kv_local, pages_local, PAGE, head_dim)
    lower_keys = jnp.min(page_keys, axis=3).astype(jnp.float32)
    upper_keys = jnp.max(page_keys, axis=3).astype(jnp.float32)
    widened = query_heads.astype(jnp.float32)
    page_bound = (
        jnp.einsum(
            "bgjd,bgpd->bgjp",
            jnp.maximum(widened, 0.0),
            upper_keys,
            precision=lax.Precision.HIGHEST,
        )
        + jnp.einsum(
            "bgjd,bgpd->bgjp",
            jnp.minimum(widened, 0.0),
            lower_keys,
            precision=lax.Precision.HIGHEST,
        )
    ) * score_scale
    page_peak = jnp.max(page_bound, axis=3)
    shard_order = jnp.arange(shards, dtype=jnp.int32)
    offset = jnp.sum(shard_counts * (shard_order < shard_index).astype(jnp.int32), axis=2)
    own_count = jnp.sum(shard_counts * (shard_order == shard_index).astype(jnp.int32), axis=2)
    slot_ids = jnp.arange(CAP, dtype=jnp.int32)
    padded = jnp.concatenate([page_list, jnp.zeros((batch_rows, kv_local, CAP), jnp.int32)], axis=2)
    picked = jnp.take_along_axis(padded, offset[:, :, None] + slot_ids, axis=2)
    slot_valid = slot_ids[None, None, :] < own_count[:, :, None]
    local_pages = jnp.where(slot_valid, picked - shard_index * pages_local, 0)
    flat_keys = key_cache.reshape(batch_rows, kv_local, pages_local, PAGE * head_dim)
    flat_values = value_cache.reshape(batch_rows, kv_local, pages_local, PAGE * head_dim)
    chosen_keys = jnp.take_along_axis(flat_keys, local_pages[:, :, :, None], axis=2).reshape(
        batch_rows, kv_local, CAP * PAGE, head_dim
    )
    chosen_values = jnp.take_along_axis(flat_values, local_pages[:, :, :, None], axis=2).reshape(
        batch_rows, kv_local, CAP * PAGE, head_dim
    )
    live_tokens = jnp.repeat(slot_valid, PAGE, axis=2)
    scores = (
        jnp.einsum("bgjd,bgtd->bgjt", query_heads, chosen_keys, preferred_element_type=jnp.float32)
        * score_scale
    )
    masked = jnp.where(live_tokens[:, :, None, :], scores, NEGATIVE)
    local_top = jnp.max(masked, axis=3)
    global_top = lax.pmax(local_top, "seq")
    page_top = lax.pmax(page_peak, "seq")
    page_terms = jnp.exp(page_bound - page_top[..., None])
    page_sum = lax.psum(jnp.sum(page_terms, axis=3), "seq")
    page_mass = (page_terms / page_sum[..., None]).reshape(
        batch_rows, kv_local * group_size, pages_local
    )
    weights = jnp.where(live_tokens[:, :, None, :], jnp.exp(masked - global_top[..., None]), 0.0)
    local_totals = jnp.sum(weights, axis=3)
    unnormed = jnp.einsum(
        "bgjt,bgtd->bgjd",
        weights.astype(jnp.bfloat16),
        chosen_values,
        preferred_element_type=jnp.float32,
    )
    head_totals = lax.psum(local_totals.reshape(batch_rows, kv_local * group_size), "seq")
    columns = lax.psum_scatter(
        unnormed.reshape(batch_rows, kv_local * group_size * head_dim),
        "seq",
        scatter_dimension=1,
        tiled=True,
    )
    column_width = columns.shape[1]
    column_heads = (
        shard_index * column_width + jnp.arange(column_width, dtype=jnp.int32)
    ) // head_dim
    selector = (
        column_heads[:, None] == jnp.arange(kv_local * group_size, dtype=jnp.int32)[None, :]
    ).astype(jnp.float32)
    column_total = jnp.dot(head_totals, selector.T, precision=lax.Precision.HIGHEST)
    attention = (columns / column_total).astype(jnp.bfloat16)
    out_terms = jnp.dot(attention, out_weight, preferred_element_type=jnp.float32)
    halfway = lax.psum_scatter(out_terms, "head", scatter_dimension=1, tiled=True)
    summed = lax.psum_scatter(halfway, "seq", scatter_dimension=1, tiled=True)
    return (summed.astype(jnp.bfloat16), attention, page_mass)


F32 = jnp.float32
BF16 = jnp.bfloat16
MESH = pl.DeviceIdType.MESH
NT = (((1,), (1,)), ((), ()))


def spread(row, first, count, offset):
    shape = (count, row.shape[1])
    sub = lax.broadcasted_iota(jnp.int32, shape, 0)
    lane = lax.broadcasted_iota(jnp.int32, shape, 1)
    return jnp.sum(jnp.where(lane == sub + (first + offset), row, 0.0), axis=1, keepdims=True)


def kernel(
    H, S,
    q_ref, list_ref, count_ref, k_hbm, v_hbm, w_hbm,
    out_ref, attn_ref, mass_ref,
    kbuf, vbuf, wbuf, qsend, qrecv, qf, hi, lo, kcat, bias, bound_buf,
    stsend, strecv, usend, urecv, psend, precv,
    ksem, vsem, wsem, qss, qrs, sss, srs, uss, urs, pss, prs,
):
    B, KV, T, HD = k_hbm.shape
    G = HQ // KVH
    PG = T // PAGE
    ROWS = B * KV * G
    CW = q_ref.shape[1]
    HO = CW // HD
    SLOTS = list_ref.shape[2]
    scale = 1.0 / math.sqrt(HD)
    h = lax.axis_index("head")
    s = lax.axis_index("seq")
    pairs = [(b, g) for b in range(B) for g in range(KV)]
    far = sorted(range(1, S), key=lambda d: -min(d, S - d))

    def seq_peer(d):
        return lax.rem(s + d, S)

    def head_peer(d):
        return lax.rem(h + d, H)

    barrier = pltpu.get_barrier_semaphore()
    for dh in range(H):
        for ds in range(S):
            if dh or ds:
                pl.semaphore_signal(
                    barrier, inc=1, device_id=(head_peer(dh), seq_peer(ds)), device_id_type=MESH
                )
    kcopies = [
        pltpu.make_async_copy(k_hbm.at[b, g], kbuf.at[n], ksem.at[n]) for n, (b, g) in enumerate(pairs)
    ]
    vcopies = [
        pltpu.make_async_copy(v_hbm.at[b, g], vbuf.at[n], vsem.at[n]) for n, (b, g) in enumerate(pairs)
    ]
    wcopy = pltpu.make_async_copy(w_hbm, wbuf, wsem)
    for c in kcopies + vcopies:
        c.start()
    wcopy.start()

    q = q_ref[...].astype(F32)
    own_q = jnp.concatenate([q[:, i * HD : (i + 1) * HD] for i in range(HO)], axis=0).astype(BF16)
    qsend[...] = own_q

    sub = lax.broadcasted_iota(jnp.int32, (len(pairs), HD), 0)
    lane = lax.broadcasted_iota(jnp.int32, (len(pairs), HD), 1)
    columns = [jnp.full((len(pairs), HD), -1, jnp.int32) for _ in range(CAP)]
    for n, (b, g) in enumerate(pairs):
        offset = jnp.int32(0)
        for j in range(S):
            offset = offset + jnp.where(j < s, count_ref[b, g, j], 0)
        own = count_ref[b, g, s]
        for c in range(CAP):
            page = list_ref[b, g, jnp.minimum(offset + c, SLOTS - 1)] - s * PG
            page = jnp.where(c < own, page, -1)
            columns[c] = jnp.where(sub == n, page, columns[c])
    for v in range(T // HD):
        pid = (lane + v * HD) // PAGE
        hit = pid == columns[0]
        for c in range(1, CAP):
            hit = hit | (pid == columns[c])
        bias[:, v * HD : (v + 1) * HD] = jnp.where(hit, 0.0, NEGATIVE)

    def bounds_of(n):
        kcopies[n].wait()
        x = kbuf[n].astype(F32).reshape(PG, 2, PAGE // 2, HD)
        hi[...] = jnp.max(x, axis=1).reshape(PG * PAGE // 2, HD)
        lo[...] = jnp.min(x, axis=1).reshape(PG * PAGE // 2, HD)
        step = PAGE // 2
        up = hi[pl.ds(0, PG, stride=step), :]
        down = lo[pl.ds(0, PG, stride=step), :]
        for i in range(1, step):
            up = jnp.maximum(up, hi[pl.ds(i, PG, stride=step), :])
            down = jnp.minimum(down, lo[pl.ds(i, PG, stride=step), :])
        kcat[n] = jnp.concatenate([up, down], axis=1).astype(BF16)

    half = len(pairs) // 2
    for n in range(half):
        bounds_of(n)

    pl.semaphore_wait(barrier, H * S - 1)

    def seq_copies(src_of, dst, send, recv):
        copies = []
        for ds in far:
            t = seq_peer(ds)
            copies.append(
                pltpu.make_async_remote_copy(
                    src_ref=src_of(t),
                    dst_ref=dst.at[s],
                    send_sem=send.at[ds],
                    recv_sem=recv.at[s],
                    device_id=(h, t),
                    device_id_type=MESH,
                )
            )
        for c in copies:
            c.start()
        return copies

    def seq_wait(src_of, dst, send, recv):
        for ds in range(1, S):
            t = seq_peer(ds)
            pltpu.make_async_remote_copy(
                src_ref=src_of(t),
                dst_ref=dst.at[t],
                send_sem=send.at[ds],
                recv_sem=recv.at[t],
                device_id=(h, t),
                device_id_type=MESH,
            ).wait_recv()

    sent = []
    q_src = lambda t: qsend
    sent += seq_copies(q_src, qrecv, qss, qrs)
    qrecv[s] = own_q
    for n in range(half, len(pairs)):
        bounds_of(n)
    seq_wait(q_src, qrecv, qss, qrs)

    qf[...] = qrecv[...].astype(F32).reshape(ROWS, HD)
    lane8 = lax.broadcasted_iota(jnp.int32, (G, HD), 1)
    sub8 = lax.broadcasted_iota(jnp.int32, (G, HD), 0)
    scores, bounds = [], []
    for n, (b, g) in enumerate(pairs):
        heads = qf[pl.ds(g * G * B + b, G, stride=B), :]
        scores.append(
            lax.dot_general(heads.astype(BF16), kbuf[n], NT, preferred_element_type=F32) * scale
            + bias[n : n + 1, :]
        )
        signed = jnp.concatenate([jnp.maximum(heads, 0.0), jnp.minimum(heads, 0.0)], axis=1)
        bounds.append(lax.dot_general(signed.astype(BF16), kcat[n], NT, preferred_element_type=F32) * scale)
    tops = [jnp.max(x, axis=1, keepdims=True) for x in scores]
    peaks = [jnp.max(x, axis=1, keepdims=True) for x in bounds]
    weights = [jnp.exp(x - m) for x, m in zip(scores, tops)]
    totals = [jnp.sum(x, axis=1, keepdims=True) for x in weights]
    sums = [jnp.sum(jnp.exp(x - m), axis=1, keepdims=True) for x, m in zip(bounds, peaks)]
    soft = jnp.zeros((G, HD), F32)
    page = jnp.zeros((G, HD), F32)
    for n in range(len(pairs)):
        first = lane8 == sub8 + n * G
        second = lane8 == sub8 + (n * G + ROWS)
        soft = jnp.where(first, tops[n], jnp.where(second, totals[n], soft))
        page = jnp.where(first, peaks[n], jnp.where(second, sums[n], page))
        bound_buf[n] = bounds[n]
    stats = jnp.concatenate(
        [jnp.sum(soft, axis=0, keepdims=True), jnp.sum(page, axis=0, keepdims=True)], axis=0
    )
    stsend[...] = stats
    st_src = lambda t: stsend
    sent += seq_copies(st_src, strecv, sss, srs)
    strecv[s] = stats

    for c in vcopies:
        c.wait()
    for n, (b, g) in enumerate(pairs):
        usend[pl.ds(g * G * B + b, G, stride=B), :] = jnp.dot(
            weights[n].astype(BF16), vbuf[n], preferred_element_type=F32
        )
    R = HO * B
    u_src = lambda t: usend.at[pl.ds(pl.multiple_of(t * R, R), R), :]
    sent += seq_copies(u_src, urecv, uss, urs)
    urecv[s] = usend[pl.ds(pl.multiple_of(s * R, R), R), :]

    seq_wait(st_src, strecv, sss, srs)
    soft_all = strecv[:, 0, :]
    page_all = strecv[:, 1, :]
    soft_scale = jnp.exp(soft_all - jnp.max(soft_all, axis=0, keepdims=True))
    soft_total = jnp.sum(pltpu.roll(soft_all, ROWS, 1) * soft_scale, axis=0, keepdims=True)
    subr = lax.broadcasted_iota(jnp.int32, (R, HD), 0)
    laner = lax.broadcasted_iota(jnp.int32, (R, HD), 1)
    mine = laner == (subr % B) * (KV * G) + s * HO + subr // B

    def column(row):
        return jnp.sum(jnp.where(mine, row, 0.0), axis=1, keepdims=True)

    factors = [column(soft_scale[p : p + 1]) for p in range(S)]
    total = column(soft_total)

    wcopy.wait()
    seq_wait(u_src, urecv, uss, urs)
    unnormed = factors[0] * urecv[0]
    for p in range(1, S):
        unnormed = unnormed + factors[p] * urecv[p]
    normed = unnormed / total
    attention = jnp.concatenate([normed[i * B : (i + 1) * B] for i in range(HO)], axis=1).astype(BF16)
    attn_ref[...] = attention

    def out_copy(dh, ts, slot):
        return pltpu.make_async_remote_copy(
            src_ref=psend.at[dh * S + ts],
            dst_ref=precv.at[slot],
            send_sem=pss.at[dh * S + ts],
            recv_sem=prs.at[slot],
            device_id=(head_peer(dh), ts),
            device_id_type=MESH,
        )

    for dh in list(range(1, H)) + [0]:
        start = pl.multiple_of(head_peer(dh) * (S * CW), S * CW)
        terms = jnp.dot(attention, wbuf[:, pl.ds(start, S * CW)], preferred_element_type=F32)
        for j in range(S):
            for i in range(HO):
                psend[dh * S + j, i * B : (i + 1) * B, :] = terms[:, j * CW + i * HD : j * CW + (i + 1) * HD]
        for ds in far + [0]:
            if dh or ds:
                c = out_copy(dh, seq_peer(ds), dh * S + s)
                c.start()
                sent.append(c)
    precv[s] = psend[s]

    page_peak = jnp.max(page_all, axis=0, keepdims=True)
    page_sum = jnp.sum(
        pltpu.roll(page_all, ROWS, 1) * jnp.exp(page_all - page_peak), axis=0, keepdims=True
    )
    for n, (b, g) in enumerate(pairs):
        peak = spread(page_peak, n * G, G, 0)
        mass = spread(page_sum, n * G, G, 0)
        mass_ref[b, g * G : (g + 1) * G, :] = jnp.exp(bound_buf[n] - peak) / mass

    for dh in range(H):
        for ds in range(S):
            if dh or ds:
                slot = dh * S + seq_peer(ds)
                out_copy(dh, seq_peer(ds), slot).wait_recv()
    summed = precv[0]
    for slot in range(1, H * S):
        summed = summed + precv[slot]
    out_ref[...] = jnp.concatenate([summed[i * B : (i + 1) * B] for i in range(HO)], axis=1).astype(BF16)
    for c in sent:
        c.wait_send()


def fused(queries, key_cache, value_cache, page_list, shard_counts, out_weight):
    B, KV, T, HD = key_cache.shape
    H, S = lax.axis_size("head"), lax.axis_size("seq")
    G = HQ // KVH
    CW = queries.shape[1]
    R = CW // HD * B
    N, PG, ROWS = B * KV, T // PAGE, B * KV * G
    vmem = pl.BlockSpec(memory_space=pltpu.VMEM)
    smem = pl.BlockSpec(memory_space=pltpu.SMEM)
    hbm = pl.BlockSpec(memory_space=pl.ANY)
    dma = pltpu.SemaphoreType.DMA
    return pl.pallas_call(
        functools.partial(kernel, H, S),
        out_shape=(
            jax.ShapeDtypeStruct((B, CW), BF16),
            jax.ShapeDtypeStruct((B, CW), BF16),
            jax.ShapeDtypeStruct((B, KV * G, PG), F32),
        ),
        in_specs=[vmem, smem, smem, hbm, hbm, hbm],
        out_specs=(vmem, vmem, vmem),
        scratch_shapes=[
            pltpu.VMEM((N, T, HD), BF16),
            pltpu.VMEM((N, T, HD), BF16),
            pltpu.VMEM(out_weight.shape, BF16),
            pltpu.VMEM((R, HD), BF16),
            pltpu.VMEM((S, R, HD), BF16),
            pltpu.VMEM((ROWS, HD), F32),
            pltpu.VMEM((T // 2, HD), F32),
            pltpu.VMEM((T // 2, HD), F32),
            pltpu.VMEM((N, PG, 2 * HD), BF16),
            pltpu.VMEM((N, T), F32),
            pltpu.VMEM((N, G, PG), F32),
            pltpu.VMEM((2, HD), F32),
            pltpu.VMEM((S, 2, HD), F32),
            pltpu.VMEM((ROWS, HD), F32),
            pltpu.VMEM((S, R, HD), F32),
            pltpu.VMEM((H * S, R, HD), F32),
            pltpu.VMEM((H * S, R, HD), F32),
            dma((N,)), dma((N,)), dma,
            dma((S,)), dma((S,)), dma((S,)), dma((S,)), dma((S,)), dma((S,)),
            dma((H * S,)), dma((H * S,)),
        ],
        compiler_params=pltpu.CompilerParams(
            collective_id=0, has_side_effects=True, vmem_limit_bytes=56 * 1024 * 1024
        ),
    )(queries, page_list, shard_counts, key_cache, value_cache, out_weight)


def whole_heads(queries, key_cache, value_cache, page_list, shard_counts, out_weight):
    B, KV, T, HD = key_cache.shape
    CW = queries.shape[1]
    rows = B * KV * (HQ // KVH)
    fits = CW % HD == 0 and (CW // HD * B) % 8 == 0 and B * KV == 8 and 2 * rows <= HD
    run = fused if fits else local
    return run(queries, key_cache, value_cache, page_list, shard_counts, out_weight)


def solution(mesh):
    return jax.shard_map(
        whole_heads,
        mesh=mesh,
        in_specs=(
            P(None, ("head", "seq")),
            P(None, "head", "seq", None),
            P(None, "head", "seq", None),
            P(None, "head", None),
            P(None, "head", None),
            P(("head", "seq"), None),
        ),
        out_specs=(P(None, ("head", "seq")), P(None, ("head", "seq")), P(None, "head", "seq")),
        check_vma=False,
    )
```

```python
import functools
import math

import jax
import jax.numpy as jnp
from jax import lax
from jax.experimental import pallas as pl
from jax.experimental.pallas import tpu as pltpu
from jax.sharding import PartitionSpec as P

HQ = 64
KVH = 8
PAGE = 16
CAP = 8


NEGATIVE = -1e30


def local(queries, key_cache, value_cache, page_list, shard_counts, out_weight):
    batch_rows, kv_local, token_count, head_dim = key_cache.shape
    group_size = HQ // KVH
    pages_local = token_count // PAGE
    shards = lax.axis_size("seq")
    shard_index = lax.axis_index("seq")
    score_scale = 1.0 / math.sqrt(head_dim)
    gathered = lax.all_gather(queries, "seq", axis=1, tiled=True)
    query_heads = gathered.reshape(batch_rows, kv_local, group_size, head_dim)
    page_keys = key_cache.reshape(batch_rows, kv_local, pages_local, PAGE, head_dim)
    lower_keys = jnp.min(page_keys, axis=3).astype(jnp.float32)
    upper_keys = jnp.max(page_keys, axis=3).astype(jnp.float32)
    widened = query_heads.astype(jnp.float32)
    page_bound = (
        jnp.einsum(
            "bgjd,bgpd->bgjp",
            jnp.maximum(widened, 0.0),
            upper_keys,
            precision=lax.Precision.HIGHEST,
        )
        + jnp.einsum(
            "bgjd,bgpd->bgjp",
            jnp.minimum(widened, 0.0),
            lower_keys,
            precision=lax.Precision.HIGHEST,
        )
    ) * score_scale
    page_peak = jnp.max(page_bound, axis=3)
    shard_order = jnp.arange(shards, dtype=jnp.int32)
    offset = jnp.sum(shard_counts * (shard_order < shard_index).astype(jnp.int32), axis=2)
    own_count = jnp.sum(shard_counts * (shard_order == shard_index).astype(jnp.int32), axis=2)
    slot_ids = jnp.arange(CAP, dtype=jnp.int32)
    padded = jnp.concatenate([page_list, jnp.zeros((batch_rows, kv_local, CAP), jnp.int32)], axis=2)
    picked = jnp.take_along_axis(padded, offset[:, :, None] + slot_ids, axis=2)
    slot_valid = slot_ids[None, None, :] < own_count[:, :, None]
    local_pages = jnp.where(slot_valid, picked - shard_index * pages_local, 0)
    flat_keys = key_cache.reshape(batch_rows, kv_local, pages_local, PAGE * head_dim)
    flat_values = value_cache.reshape(batch_rows, kv_local, pages_local, PAGE * head_dim)
    chosen_keys = jnp.take_along_axis(flat_keys, local_pages[:, :, :, None], axis=2).reshape(
        batch_rows, kv_local, CAP * PAGE, head_dim
    )
    chosen_values = jnp.take_along_axis(flat_values, local_pages[:, :, :, None], axis=2).reshape(
        batch_rows, kv_local, CAP * PAGE, head_dim
    )
    live_tokens = jnp.repeat(slot_valid, PAGE, axis=2)
    scores = (
        jnp.einsum("bgjd,bgtd->bgjt", query_heads, chosen_keys, preferred_element_type=jnp.float32)
        * score_scale
    )
    masked = jnp.where(live_tokens[:, :, None, :], scores, NEGATIVE)
    local_top = jnp.max(masked, axis=3)
    global_top = lax.pmax(local_top, "seq")
    page_top = lax.pmax(page_peak, "seq")
    page_terms = jnp.exp(page_bound - page_top[..., None])
    page_sum = lax.psum(jnp.sum(page_terms, axis=3), "seq")
    page_mass = (page_terms / page_sum[..., None]).reshape(
        batch_rows, kv_local * group_size, pages_local
    )
    weights = jnp.where(live_tokens[:, :, None, :], jnp.exp(masked - global_top[..., None]), 0.0)
    local_totals = jnp.sum(weights, axis=3)
    unnormed = jnp.einsum(
        "bgjt,bgtd->bgjd",
        weights.astype(jnp.bfloat16),
        chosen_values,
        preferred_element_type=jnp.float32,
    )
    head_totals = lax.psum(local_totals.reshape(batch_rows, kv_local * group_size), "seq")
    columns = lax.psum_scatter(
        unnormed.reshape(batch_rows, kv_local * group_size * head_dim),
        "seq",
        scatter_dimension=1,
        tiled=True,
    )
    column_width = columns.shape[1]
    column_heads = (
        shard_index * column_width + jnp.arange(column_width, dtype=jnp.int32)
    ) // head_dim
    selector = (
        column_heads[:, None] == jnp.arange(kv_local * group_size, dtype=jnp.int32)[None, :]
    ).astype(jnp.float32)
    column_total = jnp.dot(head_totals, selector.T, precision=lax.Precision.HIGHEST)
    attention = (columns / column_total).astype(jnp.bfloat16)
    out_terms = jnp.dot(attention, out_weight, preferred_element_type=jnp.float32)
    halfway = lax.psum_scatter(out_terms, "head", scatter_dimension=1, tiled=True)
    summed = lax.psum_scatter(halfway, "seq", scatter_dimension=1, tiled=True)
    return (summed.astype(jnp.bfloat16), attention, page_mass)


F32 = jnp.float32
BF16 = jnp.bfloat16
SENT = jnp.float32
EARLY = 4
TURN = True
MESH = pl.DeviceIdType.MESH
NT = (((1,), (1,)), ((), ()))


def spread(row, first, count, offset):
    shape = (count, row.shape[1])
    sub = lax.broadcasted_iota(jnp.int32, shape, 0)
    lane = lax.broadcasted_iota(jnp.int32, shape, 1)
    return jnp.sum(jnp.where(lane == sub + (first + offset), row, 0.0), axis=1, keepdims=True)


def kernel(
    H, S,
    q_hbm, list_hbm, count_hbm, k_hbm, v_hbm, w_hbm,
    sum_ref, attn_ref, mass_ref,
    q_ref, list_ref, count_ref, kbuf, kturn, vbuf, wbuf, qsend, qrecv, qf, hi, lo, kcat, bias, bound_buf,
    stsend, strecv, pgsend, pgrecv, usend, urecv, psend, precv,
    isem, ksem, vsem, wsem, qss, qrs, sss, srs, uss, urs, gss, grs, pss, prs,
):
    B, KV, T, HD = k_hbm.shape
    G = HQ // KVH
    PG = T // PAGE
    ROWS = B * KV * G
    CW = q_ref.shape[1]
    HO = CW // HD
    SLOTS = list_ref.shape[2]
    scale = 1.0 / math.sqrt(HD)
    h = lax.axis_index("head")
    s = lax.axis_index("seq")
    pairs = [(b, g) for b in range(B) for g in range(KV)]
    far = sorted(range(1, S), key=lambda d: -min(d, S - d))

    def seq_peer(d):
        return lax.rem(s + d, S)

    def head_peer(d):
        return lax.rem(h + d, H)

    barrier = pltpu.get_barrier_semaphore()
    for dh in range(H):
        for ds in range(S):
            if dh or ds:
                pl.semaphore_signal(
                    barrier, inc=1, device_id=(head_peer(dh), seq_peer(ds)), device_id_type=MESH
                )
    icopies = [
        pltpu.make_async_copy(q_hbm, q_ref, isem.at[0]),
        pltpu.make_async_copy(list_hbm, list_ref, isem.at[1]),
        pltpu.make_async_copy(count_hbm, count_ref, isem.at[2]),
    ]
    for c in icopies:
        c.start()
    kcopies = [
        pltpu.make_async_copy(k_hbm.at[b, g], kbuf.at[n], ksem.at[n]) for n, (b, g) in enumerate(pairs)
    ]
    vcopies = [
        pltpu.make_async_copy(v_hbm.at[b, g], vbuf.at[n], vsem.at[n]) for n, (b, g) in enumerate(pairs)
    ]
    wcopy = pltpu.make_async_copy(w_hbm, wbuf, wsem)
    for c in kcopies + vcopies:
        c.start()
    wcopy.start()

    for c in icopies:
        c.wait()
    q = q_ref[...].astype(F32)
    own_q = jnp.concatenate([q[:, i * HD : (i + 1) * HD] for i in range(HO)], axis=0).astype(BF16)
    qsend[...] = own_q

    sub = lax.broadcasted_iota(jnp.int32, (len(pairs), HD), 0)
    lane = lax.broadcasted_iota(jnp.int32, (len(pairs), HD), 1)
    columns = [jnp.full((len(pairs), HD), -1, jnp.int32) for _ in range(CAP)]
    for n, (b, g) in enumerate(pairs):
        offset = jnp.int32(0)
        for j in range(S):
            offset = offset + jnp.where(j < s, count_ref[b, g, j], 0)
        own = count_ref[b, g, s]
        for c in range(CAP):
            page = list_ref[b, g, jnp.minimum(offset + c, SLOTS - 1)] - s * PG
            page = jnp.where(c < own, page, -1)
            columns[c] = jnp.where(sub == n, page, columns[c])
    for v in range(T // HD):
        pid = (lane + v * HD) // PAGE
        hit = pid == columns[0]
        for c in range(1, CAP):
            hit = hit | (pid == columns[c])
        bias[:, v * HD : (v + 1) * HD] = jnp.where(hit, 0.0, NEGATIVE)

    def bounds_of(n):
        kcopies[n].wait()
        if TURN:
            kturn[n] = kbuf[n].T
        x = kbuf[n].astype(F32).reshape(PG, 2, PAGE // 2, HD)
        hi[...] = jnp.max(x, axis=1).reshape(PG * PAGE // 2, HD)
        lo[...] = jnp.min(x, axis=1).reshape(PG * PAGE // 2, HD)
        step = PAGE // 2
        up = hi[pl.ds(0, PG, stride=step), :]
        down = lo[pl.ds(0, PG, stride=step), :]
        for i in range(1, step):
            up = jnp.maximum(up, hi[pl.ds(i, PG, stride=step), :])
            down = jnp.minimum(down, lo[pl.ds(i, PG, stride=step), :])
        kcat[n] = jnp.concatenate([up, down], axis=1).astype(BF16)

    def score_of(n, heads):
        if TURN:
            return jnp.dot(heads, kturn[n], preferred_element_type=F32)
        return lax.dot_general(heads, kbuf[n], NT, preferred_element_type=F32)

    half = EARLY
    for n in range(half):
        bounds_of(n)

    pl.semaphore_wait(barrier, H * S - 1)

    def seq_copies(src_of, dst, send, recv):
        copies = []
        for ds in far:
            t = seq_peer(ds)
            copies.append(
                pltpu.make_async_remote_copy(
                    src_ref=src_of(t),
                    dst_ref=dst.at[s],
                    send_sem=send.at[ds],
                    recv_sem=recv.at[s],
                    device_id=(h, t),
                    device_id_type=MESH,
                )
            )
        for c in copies:
            c.start()
        return copies

    def seq_wait(src_of, dst, send, recv):
        for ds in range(1, S):
            t = seq_peer(ds)
            pltpu.make_async_remote_copy(
                src_ref=src_of(t),
                dst_ref=dst.at[t],
                send_sem=send.at[ds],
                recv_sem=recv.at[t],
                device_id=(h, t),
                device_id_type=MESH,
            ).wait_recv()

    sent = []
    q_src = lambda t: qsend
    sent += seq_copies(q_src, qrecv, qss, qrs)
    qrecv[s] = own_q
    for n in range(half, len(pairs)):
        bounds_of(n)
    seq_wait(q_src, qrecv, qss, qrs)

    qf[...] = qrecv[...].astype(F32).reshape(ROWS, HD)
    lane8 = lax.broadcasted_iota(jnp.int32, (G, HD), 1)
    sub8 = lax.broadcasted_iota(jnp.int32, (G, HD), 0)
    queries = [qf[pl.ds(g * G * B + b, G, stride=B), :] for b, g in pairs]
    scores = [
        score_of(n, queries[n].astype(BF16)) * scale + bias[n : n + 1, :] for n in range(len(pairs))
    ]
    tops = [jnp.max(x, axis=1, keepdims=True) for x in scores]
    weights = [jnp.exp(x - m) for x, m in zip(scores, tops)]
    totals = [jnp.sum(x, axis=1, keepdims=True) for x in weights]

    def packed(left, right):
        tile = jnp.zeros((G, HD), F32)
        for n in range(len(pairs)):
            tile = jnp.where(lane8 == sub8 + n * G, left[n], tile)
            tile = jnp.where(lane8 == sub8 + (n * G + ROWS), right[n], tile)
        return jnp.sum(tile, axis=0, keepdims=True)

    stats = packed(tops, totals)
    stsend[...] = stats
    st_src = lambda t: stsend
    sent += seq_copies(st_src, strecv, sss, srs)
    strecv[s] = stats

    for c in vcopies:
        c.wait()
    for n, (b, g) in enumerate(pairs):
        usend[pl.ds(g * G * B + b, G, stride=B), :] = jnp.dot(
            weights[n].astype(BF16), vbuf[n], preferred_element_type=F32
        )
    R = HO * B
    u_src = lambda t: usend.at[pl.ds(pl.multiple_of(t * R, R), R), :]
    sent += seq_copies(u_src, urecv, uss, urs)
    urecv[s] = usend[pl.ds(pl.multiple_of(s * R, R), R), :]

    bounds = []
    for n in range(len(pairs)):
        signed = jnp.concatenate([jnp.maximum(queries[n], 0.0), jnp.minimum(queries[n], 0.0)], axis=1)
        bounds.append(lax.dot_general(signed.astype(BF16), kcat[n], NT, preferred_element_type=F32) * scale)
        bound_buf[n] = bounds[n]
    peaks = [jnp.max(x, axis=1, keepdims=True) for x in bounds]
    sums = [jnp.sum(jnp.exp(x - m), axis=1, keepdims=True) for x, m in zip(bounds, peaks)]
    page_stats = packed(peaks, sums)
    pgsend[...] = page_stats
    pg_src = lambda t: pgsend
    sent += seq_copies(pg_src, pgrecv, gss, grs)
    pgrecv[s] = page_stats

    seq_wait(st_src, strecv, sss, srs)
    soft_all = strecv[:, 0, :]
    soft_scale = jnp.exp(soft_all - jnp.max(soft_all, axis=0, keepdims=True))
    soft_total = jnp.sum(pltpu.roll(soft_all, ROWS, 1) * soft_scale, axis=0, keepdims=True)
    subr = lax.broadcasted_iota(jnp.int32, (R, HD), 0)
    laner = lax.broadcasted_iota(jnp.int32, (R, HD), 1)
    mine = laner == (subr % B) * (KV * G) + s * HO + subr // B

    def column(row):
        return jnp.sum(jnp.where(mine, row, 0.0), axis=1, keepdims=True)

    factors = [column(soft_scale[p : p + 1]) for p in range(S)]
    total = column(soft_total)

    wcopy.wait()
    seq_wait(u_src, urecv, uss, urs)
    unnormed = factors[0] * urecv[0]
    for p in range(1, S):
        unnormed = unnormed + factors[p] * urecv[p]
    normed = unnormed / total
    attention = jnp.concatenate([normed[i * B : (i + 1) * B] for i in range(HO)], axis=1).astype(BF16)
    attn_ref[...] = attention

    def stacked(x):
        return jnp.concatenate([x[:, i * HD : (i + 1) * HD] for i in range(HO)], axis=0)

    def out_copy(dh, ts, slot):
        return pltpu.make_async_remote_copy(
            src_ref=psend.at[dh * S + ts],
            dst_ref=precv.at[slot],
            send_sem=pss.at[dh * S + ts],
            recv_sem=prs.at[slot],
            device_id=(head_peer(dh), ts),
            device_id_type=MESH,
        )

    for dh in list(range(1, H)) + [0]:
        start = pl.multiple_of(head_peer(dh) * (S * CW), S * CW)
        terms = jnp.dot(attention, wbuf[:, pl.ds(start, S * CW)], preferred_element_type=F32)
        for j in range(S):
            psend[dh * S + j] = stacked(terms[:, j * CW : (j + 1) * CW]).astype(SENT)
        for ds in far + [0]:
            if dh or ds:
                c = out_copy(dh, seq_peer(ds), dh * S + s)
                c.start()
                sent.append(c)
    precv[s] = psend[s]

    seq_wait(pg_src, pgrecv, gss, grs)
    page_all = pgrecv[:, 0, :]
    page_peak = jnp.max(page_all, axis=0, keepdims=True)
    page_sum = jnp.sum(
        pltpu.roll(page_all, ROWS, 1) * jnp.exp(page_all - page_peak), axis=0, keepdims=True
    )
    for n, (b, g) in enumerate(pairs):
        peak = spread(page_peak, n * G, G, 0)
        mass = spread(page_sum, n * G, G, 0)
        mass_ref[b, g * G : (g + 1) * G, :] = jnp.exp(bound_buf[n] - peak) / mass

    for dh in range(H):
        for ds in range(S):
            if dh or ds:
                slot = dh * S + seq_peer(ds)
                out_copy(dh, seq_peer(ds), slot).wait_recv()
    summed = precv[0].astype(F32)
    for slot in range(1, H * S):
        summed = summed + precv[slot].astype(F32)
    sum_ref[...] = summed
    for c in sent:
        c.wait_send()


def finish(sum_ref, attn_in, mass_in, out_ref, attn_ref, mass_ref):
    B, CW = out_ref.shape
    HD = sum_ref.shape[1]
    rows = sum_ref[...]
    out_ref[...] = jnp.concatenate([rows[i * B : (i + 1) * B] for i in range(CW // HD)], axis=1).astype(BF16)
    attn_ref[...] = attn_in[...]
    mass_ref[...] = mass_in[...]


def fused(queries, key_cache, value_cache, page_list, shard_counts, out_weight):
    B, KV, T, HD = key_cache.shape
    H, S = lax.axis_size("head"), lax.axis_size("seq")
    G = HQ // KVH
    CW = queries.shape[1]
    R = CW // HD * B
    N, PG, ROWS = B * KV, T // PAGE, B * KV * G
    vmem = pl.BlockSpec(memory_space=pltpu.VMEM)
    hbm = pl.BlockSpec(memory_space=pl.ANY)
    dma = pltpu.SemaphoreType.DMA
    partial_outs = pl.pallas_call(
        functools.partial(kernel, H, S),
        out_shape=(
            pltpu.VMEM((R, HD), F32),
            pltpu.VMEM((B, CW), BF16),
            pltpu.VMEM((B, KV * G, PG), F32),
        ),
        in_specs=[hbm] * 6,
        out_specs=(vmem, vmem, vmem),
        scratch_shapes=[
            pltpu.VMEM((B, CW), BF16),
            pltpu.SMEM(page_list.shape, jnp.int32),
            pltpu.SMEM(shard_counts.shape, jnp.int32),
            pltpu.VMEM((N, T, HD), BF16),
            pltpu.VMEM((N, HD, T), BF16),
            pltpu.VMEM((N, T, HD), BF16),
            pltpu.VMEM(out_weight.shape, BF16),
            pltpu.VMEM((R, HD), BF16),
            pltpu.VMEM((S, R, HD), BF16),
            pltpu.VMEM((ROWS, HD), F32),
            pltpu.VMEM((T // 2, HD), F32),
            pltpu.VMEM((T // 2, HD), F32),
            pltpu.VMEM((N, PG, 2 * HD), BF16),
            pltpu.VMEM((N, T), F32),
            pltpu.VMEM((N, G, PG), F32),
            pltpu.VMEM((1, HD), F32),
            pltpu.VMEM((S, 1, HD), F32),
            pltpu.VMEM((1, HD), F32),
            pltpu.VMEM((S, 1, HD), F32),
            pltpu.VMEM((ROWS, HD), F32),
            pltpu.VMEM((S, R, HD), F32),
            pltpu.VMEM((H * S, R, HD), SENT),
            pltpu.VMEM((H * S, R, HD), SENT),
            dma((3,)), dma((N,)), dma((N,)), dma,
            dma((S,)), dma((S,)), dma((S,)), dma((S,)), dma((S,)), dma((S,)), dma((S,)), dma((S,)),
            dma((H * S,)), dma((H * S,)),
        ],
        compiler_params=pltpu.CompilerParams(
            collective_id=0, has_side_effects=True, vmem_limit_bytes=56 * 1024 * 1024
        ),
    )(queries, page_list, shard_counts, key_cache, value_cache, out_weight)
    return pl.pallas_call(
        finish,
        out_shape=(
            jax.ShapeDtypeStruct((B, CW), BF16),
            jax.ShapeDtypeStruct((B, CW), BF16),
            jax.ShapeDtypeStruct((B, KV * G, PG), F32),
        ),
        in_specs=[vmem] * 3,
        out_specs=(vmem, vmem, vmem),
    )(*(pltpu.with_memory_space_constraint(x, pltpu.VMEM) for x in partial_outs))


def whole_heads(queries, key_cache, value_cache, page_list, shard_counts, out_weight):
    B, KV, T, HD = key_cache.shape
    CW = queries.shape[1]
    rows = B * KV * (HQ // KVH)
    fits = CW % HD == 0 and (CW // HD * B) % 8 == 0 and B * KV == 8 and 2 * rows <= HD
    run = fused if fits else local
    return run(queries, key_cache, value_cache, page_list, shard_counts, out_weight)


def solution(mesh):
    return jax.shard_map(
        whole_heads,
        mesh=mesh,
        in_specs=(
            P(None, ("head", "seq")),
            P(None, "head", "seq", None),
            P(None, "head", "seq", None),
            P(None, "head", None),
            P(None, "head", None),
            P(("head", "seq"), None),
        ),
        out_specs=(P(None, ("head", "seq")), P(None, ("head", "seq")), P(None, "head", "seq")),
        check_vma=False,
    )
```
